32 devices in a mesh: groups: 2 (over x), tp: 8 (over z, y), blk: 2 (over core).
Axes of the slice: x: 2, y: 2, z: 4, core: 2. Of those that a mesh axis runs over, the one named last changes fastest.
Arguments:
- tokens: bfloat16 [4096, 7168], P(('groups', 'tp')), parts along dimension 0, may hold values from -6 to 6
- gate_weight: bfloat16 [7168, 2048], P('tp', 'blk'), may hold values from -0.0625 to 0.0625
- up_weight: bfloat16 [7168, 2048], P('tp', 'blk'), may hold values from -0.0625 to 0.0625
- down_weight: bfloat16 [2048, 7168], P('blk', 'tp'), may hold values from -0.125 to 0.125
Outputs:
- mixed: bfloat16 [4096, 7168], P(('groups', 'blk'), 'tp'), parts along dimension 0
The draws below stay inside these ranges and needn't reach their ends.
There are 2 independent parts, one for each index of `groups`. The reference program is written for one: setup_inputs(seed, part) draws one part's arguments, and reference() takes and returns one part's arrays. A program takes and returns all parts, laid end to end along the dimension named above; an argument that names none is the same for every part. Nothing has to cross between parts.
All inputs are finite; a program needn't handle non-finite values.
Results may differ from the reference program's by a relative error of at most 0.005.
Values may be sent and summed in bfloat16 or wider, within the bound.
No kernel may reach another device: no remote copies, remote signals or barrier semaphores. Data moves between devices by JAX's collectives and lax.ppermute only.
A program may use at most 128 MiB of HBM per device.

```python
import jax
import jax.numpy as jnp

D = 7168
FF = 2048
TOKENS = 2048


def shard_levels(key, extent, shards, least, top_value):
    gain, own = 1.0, jax.random.fold_in(key, 6)
    for position, blocks in shards:
        heights = jnp.exp(jax.random.uniform(jax.random.fold_in(own, position), (blocks,), jnp.float32, least / len(shards), top_value / len(shards)))
        gain = gain * jnp.repeat(heights, extent[position] // blocks).reshape([-1 if axis == position else 1 for axis in range(len(extent))])
    return gain


def bell_draw(stream_key, shape, spread, bound, cuts=(), dtype=jnp.bfloat16):
    factor_of = shard_levels(stream_key, shape, cuts, -0.22, 0.18) if cuts else 1.0
    array = jax.random.normal(stream_key, shape, jnp.float32) * spread * factor_of
    return jnp.minimum(jnp.maximum(array, -bound), bound).astype(dtype)


def setup_inputs(seed: int = 0, part: int = 0) -> dict:
    key_list = jax.random.split(jax.random.key(seed), 5)
    own_keys = jax.random.split(jax.random.fold_in(key_list[4], part), 5)
    tokens = bell_draw(own_keys[0], (TOKENS, D), 1.0, 6.0, ((0, 8),))
    gate_weight = bell_draw(key_list[1], (D, FF), D ** -0.5, 0.0625, ((0, 8), (1, 2)))
    up_weight = bell_draw(key_list[2], (D, FF), D ** -0.5, 0.0625, ((0, 8), (1, 2)))
    down_weight = bell_draw(key_list[3], (FF, D), FF ** -0.5, 0.125, ((0, 2), (1, 8)))
    return dict(tokens=tokens, gate_weight=gate_weight, up_weight=up_weight, down_weight=down_weight)


def reference(tokens, gate_weight, up_weight, down_weight):
    gate = jnp.dot(tokens, gate_weight, preferred_element_type=jnp.float32)
    up = jnp.dot(tokens, up_weight, preferred_element_type=jnp.float32)
    hidden = (jax.nn.silu(gate) * up).astype(jnp.bfloat16)
    return jnp.dot(hidden, down_weight, preferred_element_type=jnp.float32).astype(jnp.bfloat16)
```

```python
import jax
import jax.numpy as jnp
from jax import lax
from jax.sharding import PartitionSpec as P


CHUNKS = 4
X_CHUNKS = 2
W_PIECES = 2

BF16 = jnp.bfloat16
F32 = jnp.float32


def dot(a, b):
    return jnp.dot(a, b, preferred_element_type=F32)


def solution(mesh):
    n = mesh.shape["tp"]
    rows_n = 2
    line = n // rows_n
    h = line // 2
    groups = mesh.shape["groups"]

    def index(z, y):
        return z * rows_n + y

    places = [(z, y) for z in range(line) for y in range(rows_n)]
    row_swap = [(index(z, y), index(z, 1 - y)) for z, y in places]
    half_swap = [(index(z, y), index((z + h) % line, y)) for z, y in places]

    def shift(d):
        return [(index(z, y), index(z // h * h + (z % h - d) % h, y)) for z, y in places]

    group_swap = [(g, g ^ 1) for g in range(groups)]
    core_swap = [(0, 1), (1, 0)]

    def local(tokens, gate_weight, up_weight, down_weight):
        t = tokens.shape[0]
        kl, f = gate_weight.shape
        u = f // 2
        cn = down_weight.shape[1]
        i = lax.axis_index("tp")
        y, z = i % rows_n, i // rows_n
        zh, zl = z // h, z % h
        first = lax.axis_index("groups") % 2 == 0
        g = lax.axis_index("groups") % 2
        core = lax.axis_index("blk")

        def part(p, half):
            w = lax.select(jnp.logical_xor(first, p == 1), gate_weight, up_weight)
            return lax.dynamic_slice(w, (0, half * u), (kl, u))

        def pieces(a, k):
            step = a.shape[0] // k
            return [a[j * step : (j + 1) * step] for j in range(k)]

        own = [part(0, y), part(1, y)]
        to_row = [part(0, 1 - y), part(1, 1 - y)]
        row = [[lax.ppermute(a, "tp", row_swap) for a in pieces(to_row[0], W_PIECES)]]
        far = {}
        for d in range(1, h):
            got = [lax.ppermute(a, "tp", shift(d)) for a in pieces(own[0], W_PIECES)]
            far[d, 0] = got, [lax.ppermute(a, "groups", group_swap) for a in got]
        row.append([lax.ppermute(a, "tp", row_swap) for a in pieces(to_row[1], 1)])
        for d in range(1, h):
            got = [lax.ppermute(a, "tp", shift(d)) for a in row[0]]
            far[d, 1] = got, [lax.ppermute(a, "groups", group_swap) for a in got]

        def blocks(p):
            return (
                [own[p]]
                + [a for d in range(1, h) for a in far[d, 0][p]]
                + row[p]
                + [a for d in range(1, h) for a in far[d, 1][p]]
            )

        weight = [jnp.concatenate(blocks(p), axis=0) for p in (0, 1)]

        def take(start, count, half, row_first):
            cols = []
            for r in (row_first, 1 - row_first):
                for d in range(h):
                    k = index(half * h + (zl + d) % h, r)
                    cols.append(lax.dynamic_slice(tokens, (start, k * kl), (count, kl)))
            return jnp.concatenate(cols, axis=1)

        def flip(a):
            m = a.shape[1] // 2
            return jnp.concatenate([a[:, m:], a[:, :m]], axis=1)

        tx = t // X_CHUNKS
        half_rows = tx // 2
        mine = take(0, t, zh, y)
        x_parts = []
        for c in range(X_CHUNKS):
            start = c * tx + core * half_rows
            r1 = lax.ppermute(take(start, half_rows, 1 - zh, y), "tp", half_swap)
            r2 = lax.ppermute(take(start, half_rows, zh, 1 - y), "tp", row_swap)
            r3 = lax.ppermute(flip(r1), "tp", row_swap)
            got = []
            for r in (r2, r1, r3):
                other = lax.ppermute(r, "blk", core_swap)
                got.append((lax.select(core == 0, r, other), lax.select(core == 0, other, r)))
            x_parts.append(got)

        def down_rows(half):
            return lax.dynamic_slice(down_weight, (half * u, 0), (u, cn))

        q0 = lax.ppermute(down_rows((1 - y) ^ g), "tp", row_swap)
        q1 = lax.ppermute(q0, "groups", group_swap)
        down = jnp.concatenate(
            [
                jnp.concatenate([down_rows(y), lax.select(first, q0, q1)], axis=1),
                jnp.concatenate([down_rows(1 - y), lax.select(first, q1, q0)], axis=1),
            ],
            axis=0,
        )
        down = jnp.concatenate([down, lax.ppermute(down, "blk", core_swap)], axis=0)

        rc = t // CHUNKS
        per_x = CHUNKS // X_CHUNKS
        result = jnp.zeros((h * rows_n * t, cn), BF16)
        for c in range(CHUNKS):
            xc, lo = c // per_x, (c % per_x) * rc

            def rows_of(k):
                both = jnp.concatenate(x_parts[xc][k], axis=0)
                return both[lo : lo + rc]

            keep = jnp.concatenate([mine[c * rc : (c + 1) * rc], rows_of(0)], axis=0)
            send = jnp.concatenate([rows_of(1), rows_of(2)], axis=0)
            part_send = [dot(send, w).astype(BF16) for w in weight]
            got = lax.ppermute(jnp.concatenate(part_send, axis=1), "tp", half_swap)
            s0 = dot(keep, weight[0]) + got[:, :u].astype(F32)
            s1 = dot(keep, weight[1]) + got[:, u:].astype(F32)
            gate, up = lax.select(first, s0, s1), lax.select(first, s1, s0)
            hidden = (jax.nn.silu(gate) * up).astype(BF16)
            hy = lax.ppermute(hidden[rc:], "tp", row_swap)
            h0 = jnp.concatenate([hidden[:rc], hy], axis=1)
            h1 = lax.ppermute(h0, "tp", half_swap)
            stay = lax.select(zh == core, h0, h1)
            leave = lax.select(zh == core, h1, h0)
            full = jnp.concatenate([stay, lax.ppermute(leave, "blk", core_swap)], axis=1)
            every = [full] + [lax.ppermute(full, "tp", shift(d)) for d in range(1, h)]
            every = jnp.concatenate(every, axis=0)
            out = dot(every, down).astype(BF16)
            other_row = lax.ppermute(out[:, cn:], "tp", row_swap)
            for d in range(h):
                base = (zl + d) % h * (rows_n * t) + c * rc
                a = out[d * rc : (d + 1) * rc, :cn]
                result = lax.dynamic_update_slice(result, a, (base + y * t, 0))
                a = other_row[d * rc : (d + 1) * rc]
                result = lax.dynamic_update_slice(result, a, (base + (1 - y) * t, 0))
        return result

    return jax.shard_map(
        local,
        mesh=mesh,
        in_specs=(P(("groups", "tp"), None), P("tp", "blk"), P("tp", "blk"), P("blk", "tp")),
        out_specs=P(("groups", "blk"), "tp"),
        check_vma=False,
    )
```
